32 devices in a mesh: grp: 2 (over x), pb: 8 (over z, y), ka: 2 (over core).
Axes of the slice: x: 2, y: 2, z: 4, core: 2. Of those that a mesh axis runs over, the one named last changes fastest.
Arguments:
- queries: bfloat16 [2048, 8192], P(('grp', 'pb', 'ka')), parts along dimension 0, may hold values from -2000 to 2000
- keys: bfloat16 [2048, 512], P(('grp', 'pb', 'ka')), parts along dimension 0, may hold values from -7 to 7
- values: bfloat16 [2048, 512], P(('grp', 'pb', 'ka')), parts along dimension 0, may hold values from -6 to 6
- panel_order: int32 [32], P('grp'), parts along dimension 0, may hold values from 0 to 15, as said below
- key_exp: int32 [32], P('grp'), parts along dimension 0, may hold values from -1 to 1
- value_exp: int32 [32], P('grp'), parts along dimension 0, may hold values from -1 to 1
Outputs:
- attended: bfloat16 [2048, 8192], P(('grp', 'pb', 'ka')), parts along dimension 0
The draws below stay inside these ranges and needn't reach their ends.
There are 2 independent parts, one for each index of `grp`. The reference program is written for one: setup_inputs(seed, part) draws one part's arguments, and reference() takes and returns one part's arrays. A program takes and returns all parts, laid end to end along the dimension named above; each array names one. Nothing has to cross between parts.
Inputs may be any that keep to these rules, and one draw needn't show every extreme that they name: panel_order is a permutation of the panel numbers 0 to 15.
All inputs are finite; a program needn't handle non-finite values.
Results may differ from the reference program's by a relative error of at most 0.005.
Values may be sent and summed in bfloat16 or wider, within the bound.
No kernel may reach another device: no remote copies, remote signals or barrier semaphores. Data moves between devices by JAX's collectives and lax.ppermute only.
A program may use at most 128 MiB of HBM per device.

```python
import math
import jax
import jax.numpy as jnp
from jax import lax

HQ = 64
KVH = 4
HD = 128
KD = 64
PANELS = 16
QTOK = 1024
KEYS = 1024


def layout_tables(key):
    order = jax.random.permutation(jax.random.fold_in(key, 11), KEYS // KD).astype(jnp.int32)
    powers = jax.random.randint(jax.random.fold_in(key, 12), (KEYS // KD,), -1, 2, dtype=jnp.int32)
    return (order, powers)


def raw_keys(key):
    base = jnp.clip(jax.random.normal(jax.random.fold_in(key, 13), (KEYS, KVH * HD), jnp.float32), -6.0, 6.0)
    return base.astype(jnp.bfloat16).astype(jnp.float32)


def draw_keys(key, part):
    return raw_keys(key).astype(jnp.bfloat16)


def draw_panel_order(key, part):
    return layout_tables(key)[0]


def draw_key_exp(key, part):
    return layout_tables(key)[1]


def draw_queries(key, part):
    drawn = jnp.clip(jax.random.normal(jax.random.fold_in(key, 15), (QTOK, HQ * HD), jnp.float32), -6.0, 6.0)
    return drawn.astype(jnp.bfloat16)


def plant(result, key, smallest, top_value):
    place = [jax.random.randint(jax.random.fold_in(key, axis), (), 0, length) for axis, length in enumerate(result.shape)]
    widest = result.shape.index(max(result.shape))
    next_to = place[:widest] + [(place[widest] + 1) % result.shape[widest]] + place[widest + 1:]
    return result.at[tuple(place)].set(smallest).at[tuple(next_to)].set(top_value)


def block_scale(rng, extent, split, low, high):
    factor_of, own = 1.0, jax.random.fold_in(rng, 6)
    for axis_at, parts in split:
        draws = jnp.exp(jax.random.uniform(jax.random.fold_in(own, axis_at), (parts,), jnp.float32, low / len(split), high / len(split)))
        factor_of = factor_of * jnp.repeat(draws, extent[axis_at] // parts).reshape([-1 if axis == axis_at else 1 for axis in range(len(extent))])
    return factor_of


def gaussian(key, shape, spread, bound, cuts=(), held_as=jnp.bfloat16):
    entries = spread * jax.random.normal(key, shape, jnp.float32)
    if cuts:
        entries = entries * block_scale(key, shape, cuts, -0.22, 0.18)
    return jnp.clip(entries, -bound, bound).astype(held_as)


def setup_inputs(seed: int = 0, part: int = 0) -> dict:
    seeds = jax.random.split(jax.random.key(seed), 7)
    own_keys = jax.random.split(jax.random.fold_in(seeds[6], part), 7)
    queries = draw_queries(jax.random.fold_in(jax.random.fold_in(seeds[6], part), 71), part)
    keys = draw_keys(jax.random.fold_in(jax.random.fold_in(seeds[6], part), 71), part)
    values = gaussian(own_keys[2], (KEYS, KVH * HD), 1.0, 6.0, ((0, 16),))
    panel_order = draw_panel_order(jax.random.fold_in(jax.random.fold_in(seeds[6], part), 71), part)
    key_exp = draw_key_exp(jax.random.fold_in(jax.random.fold_in(seeds[6], part), 71), part)
    value_exp = plant(jax.random.randint(own_keys[5], (PANELS,), -1, 2), jax.random.fold_in(own_keys[5], 1), -1, 1).astype(jnp.int32)
    return {"queries": queries, "keys": keys, "values": values, "panel_order": panel_order, "key_exp": key_exp, "value_exp": value_exp}


NEG_BIG = -1.0e30


def reference(queries, keys, values, panel_order, key_exp, value_exp):
    panel_count = KEYS // KD
    key_scale = jnp.exp2(key_exp.astype(jnp.float32))
    value_scale = jnp.exp2(value_exp.astype(jnp.float32))
    key_eff = (keys.astype(jnp.float32).reshape(panel_count, KD, KVH * HD) * key_scale[:, None, None]).reshape(KEYS, KVH, HD)
    value_eff = (values.astype(jnp.float32).reshape(panel_count, KD, KVH * HD) * value_scale[:, None, None]).reshape(KEYS, KVH, HD)
    key_pos = (panel_order[:, None] * KD + jnp.arange(KD, dtype=jnp.int32)[None, :]).reshape(KEYS).astype(jnp.int32)
    block_rows = math.gcd(QTOK, 128)

    def one_block(first_row):
        rows_here = lax.dynamic_slice_in_dim(queries, first_row, block_rows, 0).astype(jnp.float32)
        rows_here = rows_here.reshape(block_rows, KVH, HQ // KVH, HD)
        scores = jnp.einsum("qgeh,kgh->qgek", rows_here, key_eff, precision=lax.Precision.HIGHEST) * (HD ** -0.5)
        query_pos = (KEYS - QTOK + first_row + jnp.arange(block_rows, dtype=jnp.int32)).astype(jnp.int32)
        visible = (key_pos[None, :] <= query_pos[:, None])[:, None, None, :]
        scores = jnp.where(visible, scores, NEG_BIG)
        top = jnp.max(scores, axis=-1, keepdims=True)
        weights = jnp.where(visible, jnp.exp(scores - top), 0.0)
        total = jnp.sum(weights, axis=-1)
        rounded = lax.optimization_barrier(weights.astype(jnp.bfloat16)).astype(jnp.float32)
        mixed = jnp.einsum("qgek,kgh->qgeh", rounded, value_eff, precision=lax.Precision.HIGHEST)
        return (mixed / total[..., None]).reshape(block_rows, HQ * HD).astype(jnp.bfloat16)

    starts = jnp.arange(0, QTOK, block_rows, dtype=jnp.int32)
    return lax.map(one_block, starts).reshape(QTOK, HQ * HD)
```

```python
import functools

import jax
import jax.numpy as jnp
from jax import lax
from jax.experimental import pallas as pl
from jax.experimental.pallas import tpu as pltpu
from jax.sharding import PartitionSpec as P

HD = 128
NEG_BIG = -1e30
LOG2E = 1.4426950408889634
VMEM_LIMIT = 60 * 1024 * 1024


def panel_lookup(slot_ids, lookup_table):
    onehot = slot_ids[:, None] == jnp.arange(lookup_table.shape[0], dtype=jnp.int32)[None, :]
    return jnp.sum(jnp.where(onehot, lookup_table[None, :], 0), axis=1)


def attend_body(q_ref, key_pos_ref, query_pos_ref, *rest, kv_heads, head_group, per_step):
    blocks, out_ref = rest[:-1], rest[-1]
    rows = q_ref.shape[0]
    width = kv_heads * HD
    scale = HD ** (-0.5) * LOG2E
    hidden = jnp.where(key_pos_ref[...] <= query_pos_ref[...], 0.0, NEG_BIG).astype(jnp.float32)
    hidden = jnp.concatenate([hidden] * per_step, axis=0)
    for head in range(kv_heads):
        at = head * HD
        key_eff = jnp.concatenate([ref[:, at : at + HD] for ref in blocks], axis=0)
        at = width + head * HD
        value_eff = jnp.concatenate([ref[:, at : at + HD] for ref in blocks], axis=0)
        for first in range(0, head_group, per_step):
            columns = [(head * head_group + first + one) * HD for one in range(per_step)]
            grouped = jnp.concatenate([q_ref[:, at : at + HD] for at in columns], axis=0)
            scores = lax.dot_general(
                grouped, key_eff, (((1,), (1,)), ((), ())), preferred_element_type=jnp.float32
            )
            scores = scores + hidden
            top = jnp.max(scores, axis=-1, keepdims=True)
            weights = jnp.exp2((scores - top) * scale)
            total = jnp.sum(weights, axis=-1, keepdims=True)
            mixed = jnp.dot(
                weights.astype(jnp.bfloat16), value_eff, preferred_element_type=jnp.float32
            )
            mixed = (mixed / total).astype(jnp.bfloat16)
            for one, at in enumerate(columns):
                out_ref[:, at : at + HD] = mixed[one * rows : (one + 1) * rows]


def attend(queries, key_pos, query_pos, blocks, kv_heads):
    head_group = queries.shape[1] // (HD * kv_heads)
    per_step = max(n for n in range(1, 9) if head_group % n == 0)
    whole = pl.BlockSpec(memory_space=pltpu.VMEM)
    return pl.pallas_call(
        functools.partial(
            attend_body, kv_heads=kv_heads, head_group=head_group, per_step=per_step
        ),
        out_shape=jax.ShapeDtypeStruct(queries.shape, jnp.bfloat16),
        in_specs=[whole] * (3 + len(blocks)),
        out_specs=whole,
        compiler_params=pltpu.CompilerParams(vmem_limit_bytes=VMEM_LIMIT),
        name="attend",
    )(queries, key_pos, query_pos, *blocks)


def gather_blocks(own):
    wide = lax.axis_size("pb")
    pair = lax.axis_size("ka")
    sides = 2 if wide % 2 == 0 else 1
    line = wide // sides

    def rotate(block, by):
        pairs = [(i, sides * ((i // sides + by) % line) + i % sides) for i in range(wide)]
        return lax.ppermute(block, "pb", pairs)

    def across(block):
        return lax.ppermute(block, "pb", [(i, i ^ 1) for i in range(wide)])

    def partner(block, by):
        return lax.ppermute(block, "ka", [(i, (i + by) % pair) for i in range(pair)])

    order = sorted(range(1, line), key=lambda by: min(by, line - by))
    column = [(own, 0)] + [(rotate(own, by), by) for by in order]
    found = [(block, by, 0) for block, by in column]
    if sides == 2:
        found += [(across(block), by, 1) for block, by in column]
    return [
        (block if shift == 0 else partner(block, shift), by, flip, shift)
        for block, by, flip in found
        for shift in range(pair)
    ]


def local(queries, keys, values, panel_order, key_exp, value_exp):
    panel_len = keys.shape[0]
    kv_heads = keys.shape[1] // HD
    own_rows = queries.shape[0]
    wide, pair = lax.axis_size("pb"), lax.axis_size("ka")
    column, core = lax.axis_index("pb"), lax.axis_index("ka")
    own_slot = column * pair + core
    total_keys = panel_len * wide * pair
    total_queries = own_rows * wide * pair

    here = jnp.arange(panel_order.shape[0], dtype=jnp.int32) == own_slot
    key_scale = jnp.exp2(jnp.sum(jnp.where(here, key_exp, 0)).astype(jnp.float32))
    value_scale = jnp.exp2(jnp.sum(jnp.where(here, value_exp, 0)).astype(jnp.float32))
    own = jnp.concatenate(
        [keys * key_scale.astype(jnp.bfloat16), values * value_scale.astype(jnp.bfloat16)], axis=1
    )

    found = gather_blocks(own)
    sides = 2 if wide % 2 == 0 else 1
    line = wide // sides
    slots = jnp.stack(
        [
            (sides * ((column // sides - by) % line) + (column % sides + flip) % sides) * pair
            + (core - shift) % pair
            for _, by, flip, shift in found
        ]
    ).astype(jnp.int32)
    key_pos = (
        panel_lookup(slots, panel_order)[:, None] * panel_len
        + jnp.arange(panel_len, dtype=jnp.int32)[None, :]
    ).reshape(1, total_keys)
    query_pos = (
        total_keys
        - total_queries
        + own_slot * own_rows
        + jnp.arange(own_rows, dtype=jnp.int32)[:, None]
    )
    return attend(queries, key_pos, query_pos, [block for block, *_ in found], kv_heads)


def solution(mesh):
    placed = (
        P(("grp", "pb", "ka"), None),
        P(("grp", "pb", "ka"), None),
        P(("grp", "pb", "ka"), None),
        P("grp"),
        P("grp"),
        P("grp"),
    )
    return jax.shard_map(
        local, mesh=mesh, in_specs=placed, out_specs=P(("grp", "pb", "ka"), None), check_vma=False
    )
```
